32 devices in a mesh: win: 4 (over y, core), tile: 8 (over z, x).
Axes of the slice: x: 2, y: 2, z: 4, core: 2. Of those that a mesh axis runs over, the one named last changes fastest.
Arguments:
- state: float32 [4, 8, 5, 32, 8, 128], P('win', 'tile'), may hold values from -6 to 6
- obs_weight: float32 [4, 8, 5, 32, 8, 128], P('win', 'tile'), may hold values from 0 to 1
- trajectory: bfloat16 [4, 8, 3, 2, 32, 8, 128], P('win', 'tile'), may hold values from -0.8984375 to 0.8984375
- coupling: float32 [5, 5], replicated, may hold values from -0.9 to 0.9
- prec_scale: float32 [5, 32], replicated, may hold values from 0.5 to 2
Outputs:
- hess_vec: float32 [4, 8, 5, 32, 8, 128], P('win', 'tile')
The draws below stay inside these ranges and needn't reach their ends.
All inputs are finite; a program needn't handle non-finite values.
Results may differ from the reference program's by a relative error of at most 0.0003.
Values sent between devices are 32-bit elements; how exact they have to be, the bound alone decides.
A program may use at most 64 MiB of HBM per device.

```python
import math
import jax
import jax.numpy as jnp
from jax import lax

VARS = 5
LEVELS = 32
STEPS = 3
TY = 4
CX = 8
CY = 128
WINDOWS = 4
TILES = 8
XTILES = 2


def shard_levels(stream_key, dims, shards, low, top_value):
    def one(axis_at, blocks):
        heights = jax.random.uniform(jax.random.fold_in(jax.random.fold_in(stream_key, 6), axis_at), (blocks,), jnp.float32, low / len(shards), top_value / len(shards))
        return jnp.repeat(jnp.exp(heights), dims[axis_at] // blocks).reshape((-1,) + (1,) * (len(dims) - axis_at - 1))

    gain = one(*shards[0])
    for cut in shards[1:]:
        gain = gain * one(*cut)
    return gain


def bell_draw(stream_key, extent, scale, most, pieces=(), dtype=jnp.bfloat16):
    array = scale * jax.random.normal(stream_key, extent, jnp.float32)
    if pieces:
        array = array * shard_levels(stream_key, extent, pieces, -0.22, 0.18)
    return jnp.clip(array, -most, most).astype(dtype)


def setup_inputs(seed: int = 0) -> dict:
    streams_of = jax.random.split(jax.random.key(seed), 6)
    return {
        "state": bell_draw(streams_of[0], (WINDOWS, TILES, VARS, LEVELS, CX, CY), 1.0, 6.0, ((0, 4), (1, 8)), jnp.float32),
        "obs_weight": jnp.clip(1.0 * jax.random.uniform(streams_of[1], (WINDOWS, TILES, VARS, LEVELS, CX, CY), jnp.float32) ** shard_levels(streams_of[1], (WINDOWS, TILES, VARS, LEVELS, CX, CY), ((0, 4), (1, 8)), -0.2, 0.2), 0.0, 1.0),
        "trajectory": bell_draw(streams_of[2], (WINDOWS, TILES, STEPS, 2, LEVELS, CX, CY), 0.15, 0.8984375, ((0, 4), (1, 8))),
        "coupling": bell_draw(streams_of[3], (VARS, VARS), 0.15, 0.9, (), jnp.float32),
        "prec_scale": jnp.clip(jnp.exp(jax.random.uniform(streams_of[4], (VARS, LEVELS), jnp.float32, math.log(0.5), math.log(2.0))), 0.5, 2.0),
    }


smooth_weight = 0.2


def to_grid(blocks):
    leading = blocks.shape[1:-2]
    blocks = blocks.reshape((XTILES, TY) + leading + (CX, CY))
    blocks = jnp.moveaxis(blocks, 0, -3)
    blocks = jnp.moveaxis(blocks, 0, -2)
    return blocks.reshape(leading + (XTILES * CX, TY * CY))


def from_grid(field):
    leading = field.shape[:-2]
    field = field.reshape(leading + (XTILES, CX, TY, CY))
    field = jnp.moveaxis(field, -2, 0)
    field = jnp.moveaxis(field, -3, 0)
    return field.reshape((TILES,) + leading + (CX, CY))


def beside(field_x, field_y):
    east_side = jnp.roll(field_x, -1, axis=-2)
    west_side = jnp.roll(field_x, 1, axis=-2)
    north_edge = jnp.roll(field_y[..., :1], -CX, axis=-2)
    south_edge = jnp.roll(field_y[..., -1:], CX, axis=-2)
    north_side = jnp.concatenate([field_y[..., 1:], north_edge], axis=-1)
    south_side = jnp.concatenate([south_edge, field_y[..., :-1]], axis=-1)
    return east_side, west_side, north_side, south_side


def tangent(field, winds, coupling):
    east_side, west_side, north_side, south_side = beside(field, field)
    mixed = jnp.einsum("vw,wlxy->vlxy", coupling, field, precision=lax.Precision.HIGHEST)
    return field + winds[0] * (east_side - west_side) + winds[1] * (north_side - south_side) + mixed


def adjoint(cotangent, winds, coupling):
    east_side, west_side, north_side, south_side = beside(winds[0] * cotangent, winds[1] * cotangent)
    mixed = jnp.einsum("wv,wlxy->vlxy", coupling, cotangent, precision=lax.Precision.HIGHEST)
    return cotangent + (west_side - east_side) + (south_side - north_side) + mixed


def precision_apply(field, prec_scale):
    east_side, west_side, north_side, south_side = beside(field, field)
    stencil = (1.0 + 4.0 * smooth_weight) * field - smooth_weight * (east_side + west_side + north_side + south_side)
    return prec_scale[:, :, None, None] * stencil


def reference(state, obs_weight, trajectory, coupling, prec_scale):
    states = [to_grid(state[window]) for window in range(WINDOWS)]
    moved = []
    for window in range(WINDOWS):
        winds_all = to_grid(trajectory[window])
        field = states[window]
        for step_number in range(STEPS):
            field = tangent(field, winds_all[step_number].astype(jnp.float32), coupling)
        moved.append(field)
    weighted = []
    for window in range(WINDOWS):
        if window == 0:
            mismatch = states[0]
        else:
            mismatch = states[window] - moved[window - 1]
        weighted.append(precision_apply(mismatch, prec_scale))
    outputs = []
    for window in range(WINDOWS):
        result = weighted[window] + to_grid(obs_weight[window]) * states[window]
        if window + 1 < WINDOWS:
            winds_all = to_grid(trajectory[window])
            cotangent = weighted[window + 1]
            for step_number in reversed(range(STEPS)):
                cotangent = adjoint(cotangent, winds_all[step_number].astype(jnp.float32), coupling)
            result = result - cotangent
        outputs.append(from_grid(result))
    return jnp.stack(outputs)
```

```python
import functools

import jax
import jax.numpy as jnp
from jax import lax
from jax.experimental import pallas as pl
from jax.experimental.pallas import tpu as pltpu
from jax.sharding import PartitionSpec as P

TY = 4
GROUP = 8

smooth_weight = 0.2


def kernel(windows, tiles, state, obs, winds, coupling, prec, out,
           field, arrived, weighted, later, xs, xr, ys, yr, send, recv, wsend, wrecv):
    variables, levels, cx, cy = state.shape
    steps = winds.shape[0]
    groups = levels // GROUP
    k = lax.axis_index("win")
    t = lax.axis_index("tile")
    before_x, after_x = lax.rem(t + tiles - TY, tiles), lax.rem(t + TY, tiles)
    before_y, after_y = lax.rem(t + tiles - 1, tiles), lax.rem(t + 1, tiles)
    first, last = k == 0, k == windows - 1
    has_next, has_prev = k < windows - 1, k > 0

    barrier = pltpu.get_barrier_semaphore()
    for other in (before_x, after_x, before_y, after_y):
        pl.semaphore_signal(barrier, inc=1, device_id={"tile": other})

    @pl.when(has_next)
    def _():
        pl.semaphore_signal(barrier, inc=1, device_id={"win": k + 1})

    @pl.when(has_prev)
    def _():
        pl.semaphore_signal(barrier, inc=1, device_id={"win": k - 1})

    pl.semaphore_wait(barrier, 4 + has_next.astype(jnp.int32) + has_prev.astype(jnp.int32))

    shape = (GROUP, cx, cy)
    row = lax.broadcasted_iota(jnp.int32, shape, 1)
    lane = lax.broadcasted_iota(jnp.int32, shape, 2)
    level = lax.broadcasted_iota(jnp.int32, shape, 0)

    def copies(slot, g):
        made = []
        for side, (s, r, at, to) in enumerate((
            (xs, xr, 0, before_x), (xs, xr, 1, after_x),
            (ys, yr, 0, before_y), (ys, yr, 1, after_y),
        )):
            made.append(pltpu.make_async_remote_copy(
                src_ref=s.at[slot, at, g], dst_ref=r.at[slot, at, g],
                send_sem=send.at[slot, side, g], recv_sem=recv.at[slot, side, g],
                device_id={"tile": to},
            ))
        return made

    def cut(g):
        return pl.ds(pl.multiple_of(g * GROUP, GROUP), GROUP)

    def onward(g):
        return pltpu.make_async_remote_copy(
            src_ref=field.at[:, cut(g)], dst_ref=arrived.at[:, cut(g)],
            send_sem=wsend.at[0, g], recv_sem=wrecv.at[0, g], device_id={"win": k + 1})

    def back(g):
        return pltpu.make_async_remote_copy(
            src_ref=weighted.at[:, cut(g)], dst_ref=later.at[:, cut(g)],
            send_sem=wsend.at[1, g], recv_sem=wrecv.at[1, g], device_id={"win": k - 1})

    def ship(slot, g, fx, fy):
        low = high = None
        for v in range(variables):
            xs[slot, 0, g, v] = fx[v][:, 0, :]
            xs[slot, 1, g, v] = fx[v][:, cx - 1, :]
            here = lane == level + v * GROUP
            a = jnp.sum(jnp.where(here, fy[v][:, :, :1], 0.0), axis=0)
            b = jnp.sum(jnp.where(here, fy[v][:, :, cy - 1:], 0.0), axis=0)
            low = a if low is None else low + a
            high = b if high is None else high + b
        ys[slot, 0, g] = low
        ys[slot, 1, g] = high
        for copy in copies(slot, g):
            copy.start()

    def receive(slot, g):
        for copy in copies(slot, g):
            copy.wait_recv()

    def beside(slot, g, v, fx, fy):
        here = lane == level + v * GROUP
        north_rim = jnp.sum(jnp.where(here, yr[slot, 0, g][None], 0.0), axis=2, keepdims=True)
        south_rim = jnp.sum(jnp.where(here, yr[slot, 1, g][None], 0.0), axis=2, keepdims=True)
        east = jnp.where(row == cx - 1, xr[slot, 0, g, v][:, None, :], pltpu.roll(fx, cx - 1, 1))
        west = jnp.where(row == 0, xr[slot, 1, g, v][:, None, :], pltpu.roll(fx, 1, 1))
        north = jnp.where(lane == cy - 1, north_rim, pltpu.roll(fy, cy - 1, 2))
        south = jnp.where(lane == 0, south_rim, pltpu.roll(fy, 1, 2))
        return east, west, north, south

    def wind(n, way, g):
        return winds[n, way, cut(g)].astype(jnp.float32)

    def held(ref, g):
        return [ref[v, cut(g)] for v in range(variables)]

    def each(f):
        lax.fori_loop(0, groups, lambda g, c: (f(g), c)[1], 0)

    @pl.when(has_next)
    def _():
        @each
        def _(g):
            f = held(state, g)
            ship(0, g, f, f)

        for n in range(steps):
            @each
            def _(g, n=n):
                receive(n, g)
                f = held(state if n == 0 else field, g)
                u, w = wind(n, 0, g), wind(n, 1, g)
                new = []
                for v in range(variables):
                    e, wst, no, so = beside(n, g, v, f[v], f[v])
                    total = f[v] + u * (e - wst) + w * (no - so)
                    for b in range(variables):
                        total = total + coupling[v, b] * f[b]
                    new.append(total)
                for v in range(variables):
                    field[v, cut(g)] = new[v]
                if n < steps - 1:
                    ship(n + 1, g, new, new)
                else:
                    onward(g).start()

    @pl.when(first)
    def _():
        @each
        def _(g):
            for v in range(variables):
                arrived[v, cut(g)] = jnp.zeros(shape, jnp.float32)

    @each
    def _(g):
        @pl.when(has_prev)
        def _():
            onward(g).wait_recv()
        f = [a - b for a, b in zip(held(state, g), held(arrived, g))]
        ship(steps, g, f, f)

    @each
    def _(g):
        receive(steps, g)
        for v in range(variables):
            f = state[v, cut(g)] - arrived[v, cut(g)]
            e, wst, no, so = beside(steps, g, v, f, f)
            stencil = (1.0 + 4.0 * smooth_weight) * f - smooth_weight * (e + wst + no + so)
            for j in range(GROUP):
                weighted[v, g * GROUP + j] = prec[v, g * GROUP + j] * stencil[j]

        @pl.when(has_prev)
        def _():
            back(g).start()

    @pl.when(has_next)
    def _():
        @each
        def _(g):
            back(g).wait_recv()
            f = held(later, g)
            u, w = wind(steps - 1, 0, g), wind(steps - 1, 1, g)
            ship(steps + 1, g, [u * a for a in f], [w * a for a in f])

        for i in range(steps):
            n = steps - 1 - i
            @each
            def _(g, i=i, n=n):
                slot = steps + 1 + i
                receive(slot, g)
                f = held(later if i == 0 else out, g)
                u, w = wind(n, 0, g), wind(n, 1, g)
                new = []
                for v in range(variables):
                    e, wst, no, so = beside(slot, g, v, u * f[v], w * f[v])
                    total = f[v] + (wst - e) + (so - no)
                    for b in range(variables):
                        total = total + coupling[b, v] * f[b]
                    new.append(total)
                if n > 0:
                    for v in range(variables):
                        out[v, cut(g)] = new[v]
                    u, w = wind(n - 1, 0, g), wind(n - 1, 1, g)
                    ship(slot + 1, g, [u * a for a in new], [w * a for a in new])
                else:
                    for v in range(variables):
                        own = weighted[v, cut(g)] + obs[v, cut(g)] * state[v, cut(g)]
                        out[v, cut(g)] = own - new[v]

    @pl.when(last)
    def _():
        @each
        def _(g):
            for v in range(variables):
                out[v, cut(g)] = weighted[v, cut(g)] + obs[v, cut(g)] * state[v, cut(g)]

    def sent(slot, g):
        for copy in copies(slot, g):
            copy.wait_send()

    @each
    def _(g):
        sent(steps, g)

        @pl.when(has_next)
        def _():
            for i in range(steps):
                sent(i, g)
                sent(steps + 1 + i, g)
            onward(g).wait_send()

        @pl.when(has_prev)
        def _():
            back(g).wait_send()


def solution(mesh):
    windows, tiles = mesh.shape["win"], mesh.shape["tile"]

    def body(state, obs, trajectory, coupling, prec):
        block = state.shape[2:]
        variables, levels, cx, cy = block
        steps = trajectory.shape[2]
        slots, groups = 2 * steps + 1, levels // GROUP
        vmem = pl.BlockSpec(memory_space=pltpu.VMEM)
        smem = pl.BlockSpec(memory_space=pltpu.SMEM)
        f32 = jnp.float32
        result = pl.pallas_call(
            functools.partial(kernel, windows, tiles),
            out_shape=jax.ShapeDtypeStruct(block, f32),
            in_specs=[vmem, vmem, vmem, smem, smem],
            out_specs=vmem,
            scratch_shapes=[pltpu.VMEM(block, f32)] * 4 + [
                pltpu.VMEM((slots, 2, groups, variables, GROUP, cy), f32),
                pltpu.VMEM((slots, 2, groups, variables, GROUP, cy), f32),
                pltpu.VMEM((slots, 2, groups, cx, cy), f32),
                pltpu.VMEM((slots, 2, groups, cx, cy), f32),
                pltpu.SemaphoreType.DMA((slots, 4, groups)),
                pltpu.SemaphoreType.DMA((slots, 4, groups)),
                pltpu.SemaphoreType.DMA((2, groups)),
                pltpu.SemaphoreType.DMA((2, groups)),
            ],
            compiler_params=pltpu.CompilerParams(
                collective_id=0, has_side_effects=True, vmem_limit_bytes=40 * 2**20),
        )(state[0, 0], obs[0, 0], trajectory[0, 0], coupling, prec)
        return result[None, None]

    spec = P("win", "tile", None, None, None, None)
    return jax.shard_map(
        body, mesh=mesh,
        in_specs=(spec, spec, P("win", "tile", None, None, None, None, None), P(), P()),
        out_specs=spec, check_vma=False)
```

```python
import functools

import jax
import jax.numpy as jnp
from jax import lax
from jax.experimental import pallas as pl
from jax.experimental.pallas import tpu as pltpu
from jax.sharding import PartitionSpec as P

TY = 4
GROUP = 8

smooth_weight = 0.2


def kernel(windows, tiles, state, obs, winds, coupling, prec, out,
           field, arrived, weighted, later, xs, xr, ys, yr, send, recv, wsend, wrecv):
    variables, levels, cx, cy = state.shape
    steps = winds.shape[0]
    groups = levels // GROUP
    k = lax.axis_index("win")
    t = lax.axis_index("tile")
    before_x, after_x = lax.rem(t + tiles - TY, tiles), lax.rem(t + TY, tiles)
    before_y, after_y = lax.rem(t + tiles - 1, tiles), lax.rem(t + 1, tiles)
    first, last = k == 0, k == windows - 1
    has_next, has_prev = k < windows - 1, k > 0

    barrier = pltpu.get_barrier_semaphore()
    for other in (before_x, after_x, before_y, after_y):
        pl.semaphore_signal(barrier, inc=1, device_id={"tile": other})

    @pl.when(has_next)
    def _():
        pl.semaphore_signal(barrier, inc=1, device_id={"win": k + 1})

    @pl.when(has_prev)
    def _():
        pl.semaphore_signal(barrier, inc=1, device_id={"win": k - 1})

    pl.semaphore_wait(barrier, 4 + has_next.astype(jnp.int32) + has_prev.astype(jnp.int32))

    shape = (GROUP, cx, cy)
    row = lax.broadcasted_iota(jnp.int32, shape, 1)
    lane = lax.broadcasted_iota(jnp.int32, shape, 2)
    level = lax.broadcasted_iota(jnp.int32, shape, 0)

    def copies(slot, g):
        made = []
        for side, (s, r, at, to) in enumerate((
            (xs, xr, 0, before_x), (xs, xr, 1, after_x),
            (ys, yr, 0, before_y), (ys, yr, 1, after_y),
        )):
            made.append(pltpu.make_async_remote_copy(
                src_ref=s.at[slot, at, g], dst_ref=r.at[slot, at, g],
                send_sem=send.at[slot, side, g], recv_sem=recv.at[slot, side, g],
                device_id={"tile": to},
            ))
        return made

    def cut(g):
        return pl.ds(pl.multiple_of(g * GROUP, GROUP), GROUP)

    def onward(g):
        return pltpu.make_async_remote_copy(
            src_ref=field.at[:, cut(g)], dst_ref=arrived.at[:, cut(g)],
            send_sem=wsend.at[0, g], recv_sem=wrecv.at[0, g], device_id={"win": k + 1})

    def back(g):
        return pltpu.make_async_remote_copy(
            src_ref=weighted.at[:, cut(g)], dst_ref=later.at[:, cut(g)],
            send_sem=wsend.at[1, g], recv_sem=wrecv.at[1, g], device_id={"win": k - 1})

    def ship(slot, g, fx, fy):
        low = high = None
        for v in range(variables):
            xs[slot, 0, g, v] = fx[v][:, :1, :]
            xs[slot, 1, g, v] = fx[v][:, cx - 1:, :]
            here = lane == level + v * GROUP
            a = jnp.sum(jnp.where(here, fy[v][:, :, :1], 0.0), axis=0)
            b = jnp.sum(jnp.where(here, fy[v][:, :, cy - 1:], 0.0), axis=0)
            low = a if low is None else low + a
            high = b if high is None else high + b
        ys[slot, 0, g] = low
        ys[slot, 1, g] = high
        for copy in copies(slot, g):
            copy.start()

    def receive(slot, g):
        for copy in copies(slot, g):
            copy.wait_recv()

    def beside(slot, g, v, fx, fy):
        low, high = yr[slot, 0, g], yr[slot, 1, g]
        spread = [(low[:, p:p + 1], high[:, p:p + 1]) for p in range(v * GROUP, (v + 1) * GROUP)]
        north_rim = jnp.stack([jnp.broadcast_to(a, shape[1:]) for a, _ in spread])
        south_rim = jnp.stack([jnp.broadcast_to(b, shape[1:]) for _, b in spread])
        east = jnp.where(row == cx - 1, xr[slot, 0, g, v], pltpu.roll(fx, cx - 1, 1))
        west = jnp.where(row == 0, xr[slot, 1, g, v], pltpu.roll(fx, 1, 1))
        north = jnp.where(lane == cy - 1, north_rim, pltpu.roll(fy, cy - 1, 2))
        south = jnp.where(lane == 0, south_rim, pltpu.roll(fy, 1, 2))
        return east, west, north, south

    def wind(n, way, g):
        return winds[n, way, cut(g)].astype(jnp.float32)

    def held(ref, g):
        return [ref[v, cut(g)] for v in range(variables)]

    def each(f):
        lax.fori_loop(0, groups, lambda g, c: (f(g), c)[1], 0)

    @pl.when(has_next)
    def _():
        @each
        def _(g):
            f = held(state, g)
            ship(0, g, f, f)

        for n in range(steps):
            @each
            def _(g, n=n):
                receive(n, g)
                f = held(state if n == 0 else field, g)
                u, w = wind(n, 0, g), wind(n, 1, g)
                new = []
                for v in range(variables):
                    e, wst, no, so = beside(n, g, v, f[v], f[v])
                    total = f[v] + u * (e - wst) + w * (no - so)
                    for b in range(variables):
                        total = total + coupling[v, b] * f[b]
                    new.append(total)
                for v in range(variables):
                    field[v, cut(g)] = new[v]
                if n < steps - 1:
                    ship(n + 1, g, new, new)
                else:
                    onward(g).start()

    own_rims = jnp.where(first, 0, steps)

    @pl.when(first)
    def _():
        @each
        def _(g):
            for v in range(variables):
                arrived[v, cut(g)] = jnp.zeros(shape, jnp.float32)

    @each
    def _(g):
        @pl.when(has_prev)
        def _():
            onward(g).wait_recv()
            f = [a - b for a, b in zip(held(state, g), held(arrived, g))]
            ship(steps, g, f, f)

    @each
    def _(g):
        @pl.when(has_prev)
        def _():
            receive(steps, g)
        for v in range(variables):
            f = state[v, cut(g)] - arrived[v, cut(g)]
            e, wst, no, so = beside(own_rims, g, v, f, f)
            stencil = (1.0 + 4.0 * smooth_weight) * f - smooth_weight * (e + wst + no + so)
            for j in range(GROUP):
                weighted[v, g * GROUP + j] = prec[v, g * GROUP + j] * stencil[j]

        @pl.when(has_prev)
        def _():
            back(g).start()

    @pl.when(has_next)
    def _():
        @each
        def _(g):
            back(g).wait_recv()
            f = held(later, g)
            u, w = wind(steps - 1, 0, g), wind(steps - 1, 1, g)
            ship(steps + 1, g, [u * a for a in f], [w * a for a in f])

        for i in range(steps):
            n = steps - 1 - i
            @each
            def _(g, i=i, n=n):
                slot = steps + 1 + i
                receive(slot, g)
                f = held(later if i == 0 else out, g)
                u, w = wind(n, 0, g), wind(n, 1, g)
                new = []
                for v in range(variables):
                    e, wst, no, so = beside(slot, g, v, u * f[v], w * f[v])
                    total = f[v] + (wst - e) + (so - no)
                    for b in range(variables):
                        total = total + coupling[b, v] * f[b]
                    new.append(total)
                if n > 0:
                    for v in range(variables):
                        out[v, cut(g)] = new[v]
                    u, w = wind(n - 1, 0, g), wind(n - 1, 1, g)
                    ship(slot + 1, g, [u * a for a in new], [w * a for a in new])
                else:
                    for v in range(variables):
                        own = weighted[v, cut(g)] + obs[v, cut(g)] * state[v, cut(g)]
                        out[v, cut(g)] = own - new[v]

    @pl.when(last)
    def _():
        @each
        def _(g):
            for v in range(variables):
                out[v, cut(g)] = weighted[v, cut(g)] + obs[v, cut(g)] * state[v, cut(g)]

    def sent(slot, g):
        for copy in copies(slot, g):
            copy.wait_send()

    @each
    def _(g):
        @pl.when(has_next)
        def _():
            for i in range(steps):
                sent(i, g)
                sent(steps + 1 + i, g)
            onward(g).wait_send()

        @pl.when(has_prev)
        def _():
            back(g).wait_send()
            sent(steps, g)


def solution(mesh):
    windows, tiles = mesh.shape["win"], mesh.shape["tile"]

    def body(state, obs, trajectory, coupling, prec):
        block = state.shape[2:]
        variables, levels, cx, cy = block
        steps = trajectory.shape[2]
        slots, groups = 2 * steps + 1, levels // GROUP
        vmem = pl.BlockSpec(memory_space=pltpu.VMEM)
        smem = pl.BlockSpec(memory_space=pltpu.SMEM)
        f32 = jnp.float32
        result = pl.pallas_call(
            functools.partial(kernel, windows, tiles),
            out_shape=jax.ShapeDtypeStruct(block, f32),
            in_specs=[vmem, vmem, vmem, smem, smem],
            out_specs=vmem,
            scratch_shapes=[pltpu.VMEM(block, f32)] * 4 + [
                pltpu.VMEM((slots, 2, groups, variables, GROUP, 1, cy), f32),
                pltpu.VMEM((slots, 2, groups, variables, GROUP, 1, cy), f32),
                pltpu.VMEM((slots, 2, groups, cx, cy), f32),
                pltpu.VMEM((slots, 2, groups, cx, cy), f32),
                pltpu.SemaphoreType.DMA((slots, 4, groups)),
                pltpu.SemaphoreType.DMA((slots, 4, groups)),
                pltpu.SemaphoreType.DMA((2, groups)),
                pltpu.SemaphoreType.DMA((2, groups)),
            ],
            compiler_params=pltpu.CompilerParams(
                collective_id=0, has_side_effects=True, vmem_limit_bytes=40 * 2**20),
        )(state[0, 0], obs[0, 0], trajectory[0, 0], coupling, prec)
        return result[None, None]

    spec = P("win", "tile", None, None, None, None)
    return jax.shard_map(
        body, mesh=mesh,
        in_specs=(spec, spec, P("win", "tile", None, None, None, None, None), P(), P()),
        out_specs=spec, check_vma=False)
```
